32 devices in a mesh: dp: 8 (over z, x), vocab: 4 (over y, core).
Axes of the slice: x: 2, y: 2, z: 4, core: 2. Of those that a mesh axis runs over, the one named last changes fastest.
Arguments:
- hidden_states: bfloat16 [1024, 3584], P('dp'), may hold values from -40 to 40
- head_weight: bfloat16 [3584, 98304], P(None, ('dp', 'vocab')), as said below
- target_ids: int32 [1024], replicated, may hold values from 0 to 98303
- seq_lengths: int32 [64], P('dp'), may hold values from 1 to 16
- domain_labels: int32 [64], P('dp'), may hold values from 0 to 21
- domain_weights: float32 [22], replicated, may hold values from 0.5 to 4
Outputs:
- token_loss: float32 [1024], P('dp')
- new_weights: float32 [22], replicated
The draws below stay inside these ranges and needn't reach their ends.
Inputs may be any that keep to these rules, and one draw needn't show every extreme that they name: `head_weight`: every entry lies within 6 / sqrt(3584) of zero.
All inputs are finite; a program needn't handle non-finite values.
Results may differ from the reference program's by a relative error of at most 0.0003.
Values may be sent and summed in bfloat16 or wider, within the bound.
A program may use at most 128 MiB of HBM per device.

```python
import math
import jax
import jax.numpy as jnp
import numpy as np
from jax import lax

D = 3584
VOCAB = 98304
SEQ_LEN = 16
DOMAINS = 22
SEQS = 64
TOKENS = 1024
N_DP = 8


def weight_table(key):
    base = jax.random.normal(jax.random.fold_in(key, 11), (D, VOCAB), jnp.float32)
    return jnp.clip(base, -6.0, 6.0) / math.sqrt(D)


def draw_head_weight(key, part):
    return weight_table(key).astype(jnp.bfloat16)


def draw_hidden_states(key, part):
    base = jax.random.normal(jax.random.fold_in(key, 31), (TOKENS, D), jnp.float32)
    return jnp.clip(3.0 * base, -18.0, 18.0).astype(jnp.bfloat16)


def plant(entries, own_key, least, high):
    dims = entries.shape
    spot = [jax.random.randint(jax.random.fold_in(own_key, axis), (), 0, dims[axis]) for axis in range(len(dims))]
    entries = entries.at[tuple(spot)].set(least)
    longest = dims.index(max(dims))
    spot[longest] = (spot[longest] + 1) % dims[longest]
    return entries.at[tuple(spot)].set(high)


def cumulative_ranks(number_of, lean):
    portions = [(1 << 20) // math.isqrt(standing ** lean) + 1 for standing in range(1, number_of + 1)]
    deviation = 1 + sum(portions) // (1 << 30)
    return np.cumsum(np.array([max(1, weight // deviation) for weight in portions]))


def skewed_ids(stream_key, extent, count, lean):
    grid = cumulative_ranks(count, lean)
    lot = jax.random.randint(jax.random.fold_in(stream_key, 1), extent, 0, int(grid[count - 1]))
    grade = jnp.searchsorted(jnp.asarray(grid, jnp.int32), lot, side="right")
    return jax.random.permutation(jax.random.fold_in(stream_key, 2), count)[grade].astype(jnp.int32)


def setup_inputs(seed: int = 0) -> dict:
    seeds = jax.random.split(jax.random.key(seed), 7)
    hidden_states = draw_hidden_states(jax.random.fold_in(seeds[6], 71), 0)
    head_weight = draw_head_weight(jax.random.fold_in(seeds[6], 71), 0)
    target_ids = plant(jax.random.randint(seeds[2], (TOKENS,), 0, VOCAB), jax.random.fold_in(seeds[2], 1), 0, VOCAB - 1).astype(jnp.int32)
    seq_lengths = plant(jax.random.randint(seeds[3], (SEQS,), 1, SEQ_LEN + 1), jax.random.fold_in(seeds[3], 1), 1, SEQ_LEN).astype(jnp.int32)
    domain_labels = plant(skewed_ids(seeds[4], (SEQS,), DOMAINS, 2), jax.random.fold_in(seeds[4], 3), 0, DOMAINS - 1).astype(jnp.int32)
    domain_weights = jnp.clip(jnp.exp(jax.random.uniform(seeds[5], (DOMAINS,), jnp.float32, math.log(0.5), math.log(4.0))), 0.5, 4.0)
    return dict(hidden_states=hidden_states, head_weight=head_weight, target_ids=target_ids, seq_lengths=seq_lengths, domain_labels=domain_labels, domain_weights=domain_weights)


explore_share = 0.01
step_rate = 0.002


def reference(hidden_states, head_weight, target_ids, seq_lengths, domain_labels, domain_weights):
    def block_loss(block):
        block_rows, targets = block
        logits = jnp.dot(block_rows, head_weight, preferred_element_type=jnp.float32)
        row_peak = jnp.max(logits, axis=1)
        mass_sum = jnp.sum(jnp.exp(logits - row_peak[:, None]), axis=1)
        picked = jnp.take_along_axis(logits, targets[:, None], axis=1)[:, 0]
        return jnp.log(mass_sum) + row_peak - picked

    blocks = (hidden_states.reshape(N_DP, -1, D), target_ids.reshape(N_DP, -1))
    raw_loss = lax.map(block_loss, blocks).reshape(-1)
    positions = jnp.arange(TOKENS) % SEQ_LEN
    valid = positions < jnp.repeat(seq_lengths, SEQ_LEN)
    token_loss = jnp.where(valid, raw_loss, 0.0)
    seq_loss = jnp.sum(token_loss.reshape(-1, SEQ_LEN), axis=1)
    seq_tokens = seq_lengths.astype(jnp.float32)
    domain_hot = (domain_labels[:, None] == jnp.arange(DOMAINS)[None, :]).astype(jnp.float32)
    domain_loss = jnp.sum(domain_hot * seq_loss[:, None], axis=0)
    domain_count = jnp.sum(domain_hot * seq_tokens[:, None], axis=0)
    probability = (1.0 - DOMAINS * explore_share) * domain_weights / jnp.sum(domain_weights) + explore_share
    reward = domain_loss / jnp.maximum(domain_count, 1.0) / probability
    raised = domain_weights * jnp.exp(step_rate * reward)
    new_weights = DOMAINS * raised / jnp.sum(raised)
    return token_loss, new_weights
```

```python
import functools
import heapq
import math

import jax
import jax.numpy as jnp
from jax import lax
from jax.experimental import pallas as pl
from jax.experimental.pallas import tpu as pltpu
from jax.sharding import PartitionSpec as P

SEQ_LEN = 16
DOMAINS = 22
LANES = 128
DOM_PAD = 24
CORES = 2
LOW = -1e30
HALVES = 1

explore_share = 0.01
step_rate = 0.002


def nearest(p, i, n):
    if isinstance(p, int):
        q = min(p, n - 1 - p)
        k = (i + 1) // 2
        at = i if i > 2 * q else q + k if i % 2 else q - k
        return at if p == q else n - 1 - at
    if i == 0:
        return p
    if n == 2:
        return 1 - p
    q = jnp.minimum(p, n - 1 - p)
    k = (i + 1) // 2
    at = jnp.where(i > 2 * q, i, q + k if i % 2 else q - k)
    return jnp.where(p == q, at, n - 1 - at)


def y_first(i, Z):
    return i in YF or i == Z - 1


YF = (0, 1)
WIRE, LATE, CORE_LATE, TICK, FIRST, OWN_END, START = 4.92, 1.8, 1.4, 1.1, 3.0, 8.5, 2.0


def plan(Z, X, Y, H, TI):
    roles = range((Z + 1) // 2)
    if X != 2 or Y != 2:
        order = sorted(((i, t) for i in range(Z) for t in range(X)), key=lambda g: (2 * g[0] + 3 * g[1], g))
        steps = []
        for k, (i, t) in enumerate(order):
            if k:
                steps += [(k * TI, ("piece", i, t, s, h)) for s in range(Y) for h in range(H)]
                steps.append((k * TI, ("core", i, t)))
        return [(order, steps) for _ in roles]
    wire = WIRE / H
    rank = [{nearest(z, i, Z): i for i in range(Z)} for z in range(Z)]
    heap, count = [], [0]

    def post(at, *what):
        count[0] += 1
        heapq.heappush(heap, (at, count[0], what))

    free = {}

    def send(at, z, link, piece):
        zs, t, s, h = piece
        done = max(at, free.get((z, link), 0.0)) + wire
        free[z, link] = done
        to = {"up": z + 1, "down": z - 1}.get(link, z)
        post(done + LATE, "piece", to, (zs, t ^ (link == "x"), s ^ (link == "y"), h), link)

    def along(at, z, zs, piece):
        if z + 1 < Z and zs <= z:
            send(at, z, "up", piece)
        if z > 0 and zs >= z:
            send(at, z, "down", piece)

    inbox = [[] for _ in range(Z)]
    left = [{(i, t): 4 * H for i in range(Z) for t in range(2) if i or t} for _ in range(Z)]
    order = [[(0, 0)] for _ in range(Z)]
    steps = [[] for _ in range(Z)]
    tick, idle = [0] * Z, [False] * Z
    for z in range(Z):
        for h in range(H):
            along(START, z, z, (z, 0, 0, h))
            send(START, z, "x", (z, 0, 0, h))
        for h in range(H):
            send(START, z, "x", (z, 0, 1, h))
        post(FIRST, "free", z)

    def work(at, z):
        while inbox[z]:
            (zs, t, s, h), link = inbox[z].pop(0)
            i = rank[z][zs]
            steps[z].append((tick[z], ("piece", i, t, s, h)))
            piece = (zs, t, s, h)
            if link in ("up", "down"):
                along(at, z, zs, piece) if zs != z else None
                send(at, z, "y", piece)
                send(at, z, "x", piece)
            elif link == "y" and t == 0 and y_first(i, Z):
                send(at, z, "x", piece)
            elif link == "x" and s == 0 and i and not y_first(i, Z):
                send(at, z, "y", piece)
            left[z][i, t] -= 1
            post(at + CORE_LATE, "core", z, (i, t))
        n = tick[z]
        if n < TI:
            tick[z] += 1
            post(max(at + TICK, OWN_END * (n + 1) / TI), "free", z)
            return
        if n % TI == 0:
            ready = [g for g in left[z] if left[z][g] == 0 and g not in order[z]]
            if not ready:
                idle[z] = True
                return
            order[z].append(ready[0])
            steps[z].append((n, ("core",) + ready[0]))
        tick[z] += 1
        post(at + TICK, "free", z)

    while heap:
        at, _, what = heapq.heappop(heap)
        z = what[1]
        if what[0] == "piece":
            inbox[z].append(what[2:])
        elif what[0] == "core":
            left[z][what[2]] -= 1
        if what[0] == "free" or idle[z]:
            if len(order[z]) == 2 * Z and tick[z] == 2 * Z * TI:
                continue
            idle[z] = False
            work(at, z)
    return [(order[z], steps[z]) for z in roles]


def kernel(Z, X, Y, H, tok, cols, TN, U,
           hid_ref, w_ref, tgt_ref, len_ref, lab_ref, dw_ref,
           loss_ref, new_ref,
           buf, w_buf, lg, off_ref, m_ref, s_ref, p_ref,
           stat_out, stat_in, dom_out, dom_in,
           own_sem, w_sem, recv_sem, send_sem, st_send, st_recv, dm_send, dm_recv):
    nv = Y * CORES
    dp = Z * X
    ndev = dp * nv
    T = cols // TN
    TI = T // U
    NG = Z * X
    pr = tok // (nv * H)
    me = lax.axis_index("dp")
    v = lax.axis_index("vocab")
    z, x = me // X, me % X
    y, c = v // CORES, v % CORES

    own_copy = pltpu.make_async_copy(hid_ref, buf.at[pl.ds(pl.multiple_of(me * tok, tok), tok)], own_sem)
    own_copy.start()

    def w_copy(j):
        return pltpu.make_async_copy(
            w_ref.at[:, pl.ds(pl.multiple_of(j * TN, TN), TN)], w_buf.at[j], w_sem.at[j]
        )

    for j in range(T):
        w_copy(j).start()

    bar = pltpu.get_barrier_semaphore()
    for d in range(dp):
        for k in range(nv):
            @pl.when((d != me) | (v != k))
            def _():
                pl.semaphore_signal(bar, inc=1, device_id=(d, k), device_id_type=pl.DeviceIdType.MESH)

    def remote(kind, zs, xs, ys, cs, h, to):
        piece = (((zs * X + xs) * Y + ys) * CORES + cs) * H + h
        rows = buf.at[pl.ds(pl.multiple_of(piece * pr, pr), pr)]
        return pltpu.make_async_remote_copy(
            src_ref=rows, dst_ref=rows,
            send_sem=send_sem.at[kind, piece], recv_sem=recv_sem.at[piece],
            device_id=to, device_id_type=pl.DeviceIdType.MESH,
        )

    def push(drain, cond, *what):
        def go():
            r = remote(*what)
            if drain:
                r.wait_send()
            else:
                r.start()
        if cond is None:
            go()
        else:
            pl.when(cond)(go)

    def dev(z_, x_, y_, c_):
        return (z_ * X + x_, y_ * CORES + c_)

    def arrive(drain, zs, xs, ys, cs, h):
        if not drain:
            remote(0, zs, xs, ys, cs, h, dev(z, x, y, 1 - c)).wait_recv()

    def line(drain, kind, n, pos, src, at, piece):
        if n == 1:
            return
        up, down = pos + 1 < n, pos > 0
        if src is not None:
            if n == 2:
                return
            up, down = up & (src < pos), down & (src > pos)
        if n == 2:
            push(drain, None, kind, *piece, at(1 - pos))
            return
        push(drain, up, kind, *piece, at(pos + 1))
        push(drain, down, kind + 1, *piece, at(pos - 1))

    def send_z(drain, src, piece):
        line(drain, 1, Z, z, src, lambda q: dev(q, x, y, c), piece)

    def send_x(drain, src, piece):
        line(drain, 3, X, x, src, lambda q: dev(z, q, y, c), piece)

    def send_y(drain, src, piece):
        line(drain, 5, Y, y, src, lambda q: dev(z, x, q, c), piece)

    def send_c(drain, piece):
        push(drain, None, 0, *piece, dev(z, x, y, 1 - c))

    def begin(drain):
        for h in range(H):
            send_z(drain, None, (z, x, y, c, h))
            send_x(drain, None, (z, x, y, c, h))
        for k in range(1, Y):
            for h in range(H):
                send_x(drain, None, (z, x, nearest(y, k, Y), c, h))

    def piece_step(drain, i, t, s, h):
        zs, xs, ys = nearest(z, i, Z), nearest(x, t, X), nearest(y, s, Y)
        piece = (zs, xs, ys, c, h)
        arrive(drain, *piece)
        if t == 0 and s == 0:
            send_z(drain, zs, piece)
            send_y(drain, None, piece)
            send_x(drain, None, piece)
        elif t == 0:
            send_y(drain, ys, piece)
            if y_first(i, Z):
                send_x(drain, None, piece)
        elif s == 0:
            send_x(drain, xs, piece)
            if not y_first(i, Z):
                send_y(drain, None, piece)
        elif y_first(i, Z):
            send_x(drain, xs, piece)
        else:
            send_y(drain, ys, piece)
        send_c(drain, piece)

    def core_step(drain, i, t):
        zs, xs = nearest(z, i, Z), nearest(x, t, X)
        for ys in range(Y):
            for h in range(H):
                arrive(drain, zs, xs, ys, 1 - c, h)

    def run(drain, what):
        kind, *at = what
        (piece_step if kind == "piece" else core_step)(drain, *at)

    plans = plan(Z, X, Y, H, TI)
    role = jnp.minimum(z, Z - 1 - z)
    ids = [nearest(z, i, Z) * X + nearest(x, t, X) for i, t in plans[0][0]]
    for r in range(1, len(plans)):
        ids = [jnp.where(role == r, nearest(z, i, Z) * X + nearest(x, t, X), g)
               for (i, t), g in zip(plans[r][0], ids)]

    def take(q):
        def at_tick(whats):
            for what in whats:
                run(False, what)

        def of_role(steps):
            for at in sorted({at for at, _ in steps}):
                pl.when(q == at)(functools.partial(at_tick, [w for n, w in steps if n == at]))

        if all(p == plans[0] for p in plans):
            of_role(plans[0][1])
        else:
            for r, (_, steps) in enumerate(plans):
                pl.when(role == r)(functools.partial(of_role, steps))

    def group(k):
        g = ids[0]
        for n in range(1, NG):
            g = jnp.where(k == n, ids[n], g)
        return g

    col_start = (me * nv + v) * cols
    lane_t = lax.broadcasted_iota(jnp.int32, (LANES, LANES), 1)
    for g in range(dp * tok // LANES):
        rows = pl.ds(g * LANES, LANES)
        ids_row = jnp.broadcast_to(tgt_ref[g:g + 1, :], (LANES, LANES))
        off_ref[rows, :] = jnp.transpose(ids_row) - lane_t - col_start
    m_ref[...] = jnp.full(m_ref.shape, LOW, jnp.float32)
    s_ref[...] = jnp.zeros(s_ref.shape, jnp.float32)
    p_ref[...] = jnp.zeros(p_ref.shape, jnp.float32)
    lg[U - 1] = jnp.full((tok, TN), 3 * LOW, jnp.float32)

    pl.semaphore_wait(bar, ndev - 1)
    own_copy.wait()
    begin(False)

    def epilogue(slot, g, col):
        rows = pl.ds(pl.multiple_of(g * tok, tok), tok)
        off = off_ref[rows, :] - col
        m_old = m_ref[rows, :]
        parts = [lg[slot, :, n * LANES:(n + 1) * LANES] for n in range(TN // LANES)]
        m_new = m_old
        for a in parts:
            m_new = jnp.maximum(m_new, a)
        s = s_ref[rows, :] * jnp.exp(m_old - m_new)
        pk = p_ref[rows, :]
        for n, a in enumerate(parts):
            s = s + jnp.exp(a - m_new)
            pk = pk + jnp.where(off == n * LANES, a, 0.0)
        m_ref[rows, :] = m_new
        s_ref[rows, :] = s
        p_ref[rows, :] = pk

    row8 = lax.broadcasted_iota(jnp.int32, (8, tok), 0)

    def finish(g):
        rows = pl.ds(pl.multiple_of(g * tok, tok), tok)
        mt = jnp.transpose(m_ref[rows, :])
        st = jnp.transpose(s_ref[rows, :])
        pt = jnp.transpose(p_ref[rows, :])
        row_m = jnp.max(mt, axis=0, keepdims=True)
        row_s = jnp.sum(st * jnp.exp(mt - row_m), axis=0, keepdims=True)
        row_p = jnp.sum(pt, axis=0, keepdims=True)
        stat_out[g] = jnp.where(row8 == 0, row_m, jnp.where(row8 == 1, row_s, row_p))

        @pl.when(g == me)
        def _():
            stat_in[me * nv + v] = stat_out[me]

        for k in range(nv):
            @pl.when((g != me) | (v != k))
            def _():
                pltpu.make_async_remote_copy(
                    src_ref=stat_out.at[g], dst_ref=stat_in.at[me * nv + v],
                    send_sem=st_send, recv_sem=st_recv,
                    device_id=(g, k), device_id_type=pl.DeviceIdType.MESH,
                ).start()

    def tick(q, _):
        k = q // TI
        i = q - k * TI
        take(q)

        @pl.when(k == 0)
        def _():
            for u in range(U):
                w_copy(i * U + u).wait()

        @pl.when(((q - 1) % TI == 0) & (q > TI))
        def _():
            finish(group((q - 1) // TI - 1))

        g = group(k)
        rows = pl.ds(pl.multiple_of(g * tok, tok), tok)
        for u in range(U):
            j = i * U + u
            if u == 0:
                g_old = jnp.where(i == 0, group(jnp.maximum(k - 1, 0)), g)
                col = jnp.where(q == 0, -(1 << 30), jnp.where(i == 0, (T - 1) * TN, (j - 1) * TN))
                epilogue(U - 1, g_old, col)
            else:
                epilogue(u - 1, g, (j - 1) * TN)
            lg[u] = jnp.dot(buf[rows, :], w_buf[j], preferred_element_type=jnp.float32)
        return 0

    lax.fori_loop(0, NG * TI, tick, 0)
    epilogue(U - 1, ids[NG - 1], (T - 1) * TN)
    for k in range(NG):
        if (k + 1) * TI + 1 >= NG * TI:
            finish(ids[k])

    begin(True)
    for _, what in plans[0][1]:
        run(True, what)

    seq = lax.broadcasted_iota(jnp.int32, (1, tok), 1)
    lens = jnp.zeros((1, tok), jnp.int32)
    labs = jnp.zeros((1, tok), jnp.int32)
    for n in range(tok // SEQ_LEN):
        mine = seq // SEQ_LEN == n
        lens = jnp.where(mine, len_ref[n], lens)
        labs = jnp.where(mine, lab_ref[n], labs)
    dom_row = lax.broadcasted_iota(jnp.int32, (DOM_PAD, LANES), 0)
    live = dom_row < DOMAINS
    weights = jnp.zeros((DOM_PAD, LANES), jnp.float32)
    for n in range(DOMAINS):
        weights = jnp.where(dom_row == n, dw_ref[n], weights)
    probability = (1.0 - DOMAINS * explore_share) * weights / jnp.sum(
        weights, axis=0, keepdims=True) + explore_share

    others = stat_in.at[pl.ds(0, ndev - 1)]
    pltpu.make_async_copy(others, others, st_recv).wait()
    ms = stat_in[:, 0, :]
    peak = jnp.max(ms, axis=0, keepdims=True)
    mass = jnp.sum(stat_in[:, 1, :] * jnp.exp(ms - peak), axis=0, keepdims=True)
    pick = jnp.sum(stat_in[:, 2, :], axis=0, keepdims=True)
    valid = seq % SEQ_LEN < lens
    loss = jnp.where(valid, jnp.log(mass) + peak - pick, 0.0)
    loss_ref[...] = loss
    dom = lax.broadcasted_iota(jnp.int32, (DOM_PAD, tok), 0)
    hot = dom == labs
    d_loss = jnp.sum(jnp.where(hot, loss, 0.0), axis=1, keepdims=True)
    d_count = jnp.sum(jnp.where(hot & valid, 1.0, 0.0), axis=1, keepdims=True)
    dlane = lax.broadcasted_iota(jnp.int32, (DOM_PAD, LANES), 1)
    dom_out[...] = jnp.where(dlane == 0, d_loss, jnp.where(dlane == 1, d_count, 0.0))
    dom_in[me] = dom_out[...]
    for k in range(1, dp):
        pltpu.make_async_remote_copy(
            src_ref=dom_out, dst_ref=dom_in.at[me],
            send_sem=dm_send, recv_sem=dm_recv,
            device_id=((me + k) % dp, v), device_id_type=pl.DeviceIdType.MESH,
        ).start()
    pltpu.make_async_copy(others, others, st_send).wait()

    rest = dom_in.at[pl.ds(0, dp - 1)]
    pltpu.make_async_copy(rest, rest, dm_recv).wait()
    total = jnp.sum(dom_in[...], axis=0)
    dom_loss = jnp.sum(jnp.where(dlane == 0, total, 0.0), axis=1, keepdims=True)
    dom_count = jnp.sum(jnp.where(dlane == 1, total, 0.0), axis=1, keepdims=True)
    reward = dom_loss / jnp.maximum(dom_count, 1.0) / probability
    raised = jnp.where(live, weights * jnp.exp(step_rate * reward), 0.0)
    new_ref[...] = DOMAINS * raised / jnp.sum(raised, axis=0, keepdims=True)
    pltpu.make_async_copy(rest, rest, dm_send).wait()


def body(hidden_states, head_weight, target_ids, seq_lengths, domain_labels, domain_weights):
    tok, width = hidden_states.shape
    cols = head_weight.shape[1]
    dp = lax.axis_size("dp")
    nv = lax.axis_size("vocab")
    X = math.isqrt(dp // 2)
    Z = dp // X
    Y = nv // CORES
    tokens = dp * tok
    TN = next(n for n in (4 * LANES, 3 * LANES, 2 * LANES, LANES) if cols % n == 0)
    T = cols // TN
    U = 2 if T % 2 == 0 else 1
    H = HALVES if tok // (nv * HALVES) >= 16 else 1
    hbm = pl.BlockSpec(memory_space=pl.ANY)
    vmem = pl.BlockSpec(memory_space=pltpu.VMEM)
    smem = pl.BlockSpec(memory_space=pltpu.SMEM)
    f32 = jnp.float32
    dma = pltpu.SemaphoreType.DMA
    loss, new = pl.pallas_call(
        functools.partial(kernel, Z, X, Y, H, tok, cols, TN, U),
        out_shape=(jax.ShapeDtypeStruct((1, tok), f32), jax.ShapeDtypeStruct((DOM_PAD, LANES), f32)),
        in_specs=[hbm, hbm, vmem, smem, smem, smem],
        out_specs=(vmem, vmem),
        scratch_shapes=[
            pltpu.VMEM((tokens, width), hidden_states.dtype),
            pltpu.VMEM((T, width, TN), head_weight.dtype),
            pltpu.VMEM((U, tok, TN), f32),
            pltpu.VMEM((tokens, LANES), jnp.int32),
            pltpu.VMEM((tokens, LANES), f32),
            pltpu.VMEM((tokens, LANES), f32),
            pltpu.VMEM((tokens, LANES), f32),
            pltpu.VMEM((dp, 8, tok), f32),
            pltpu.VMEM((dp * nv, 8, tok), f32),
            pltpu.VMEM((DOM_PAD, LANES), f32),
            pltpu.VMEM((dp, DOM_PAD, LANES), f32),
            dma(()),
            dma((T,)),
            dma((dp * nv * H,)),
            dma((7, dp * nv * H)),
            dma(()), dma(()), dma(()), dma(()),
        ],
        compiler_params=pltpu.CompilerParams(
            has_side_effects=True, collective_id=0, vmem_limit_bytes=60 * 2**20),
    )(hidden_states, head_weight, target_ids.reshape(tokens // LANES, LANES), seq_lengths, domain_labels,
      domain_weights)
    return loss[0], new[:DOMAINS, 0]


def solution(mesh):
    placed = (P("dp", None), P(None, ("dp", "vocab")), P(), P("dp"), P("dp"), P())
    return jax.shard_map(
        body, mesh=mesh, in_specs=placed, out_specs=(P("dp"), P()), check_vma=False
    )
```

```python
import functools
import heapq
import math

import jax
import jax.numpy as jnp
from jax import lax
from jax.experimental import pallas as pl
from jax.experimental.pallas import tpu as pltpu
from jax.sharding import PartitionSpec as P

SEQ_LEN = 16
DOMAINS = 22
LANES = 128
CORES = 2
LOW = -1e30
HALVES = 1

explore_share = 0.01
step_rate = 0.002


def nearest(p, i, n):
    if isinstance(p, int):
        q = min(p, n - 1 - p)
        k = (i + 1) // 2
        at = i if i > 2 * q else q + k if i % 2 else q - k
        return at if p == q else n - 1 - at
    if i == 0:
        return p
    if n == 2:
        return 1 - p
    q = jnp.minimum(p, n - 1 - p)
    k = (i + 1) // 2
    at = jnp.where(i > 2 * q, i, q + k if i % 2 else q - k)
    return jnp.where(p == q, at, n - 1 - at)


def y_first(i, Z):
    return i in YF or i == Z - 1


YF = (0, 1)
WIRE, LATE, CORE_LATE, TICK, FIRST, OWN_END, START = 4.92, 2.2, 1.6, 1.14, 3.0, 9.0, 3.5


def plan(Z, X, Y, H, TI):
    roles = range((Z + 1) // 2)
    if X != 2 or Y != 2:
        order = sorted(((i, t) for i in range(Z) for t in range(X)), key=lambda g: (2 * g[0] + 3 * g[1], g))
        steps = []
        for k, (i, t) in enumerate(order):
            if k:
                steps += [(k * TI, ("piece", i, t, s, h)) for s in range(Y) for h in range(H)]
                steps.append((k * TI, ("core", i, t)))
        return [(order, steps) for _ in roles]
    wire = WIRE / H
    rank = [{nearest(z, i, Z): i for i in range(Z)} for z in range(Z)]
    heap, count = [], [0]

    def post(at, *what):
        count[0] += 1
        heapq.heappush(heap, (at, count[0], what))

    free = {}

    def send(at, z, link, piece):
        zs, t, s, h = piece
        done = max(at, free.get((z, link), 0.0)) + wire
        free[z, link] = done
        to = {"up": z + 1, "down": z - 1}.get(link, z)
        post(done + LATE, "piece", to, (zs, t ^ (link == "x"), s ^ (link == "y"), h), link)

    def along(at, z, zs, piece):
        if z + 1 < Z and zs <= z:
            send(at, z, "up", piece)
        if z > 0 and zs >= z:
            send(at, z, "down", piece)

    inbox = [[] for _ in range(Z)]
    left = [{(i, t): 4 * H for i in range(Z) for t in range(2) if i or t} for _ in range(Z)]
    order = [[(0, 0)] for _ in range(Z)]
    steps = [[] for _ in range(Z)]
    tick, idle = [0] * Z, [False] * Z
    for z in range(Z):
        for h in range(H):
            along(START, z, z, (z, 0, 0, h))
            send(START, z, "x", (z, 0, 0, h))
        for h in range(H):
            send(START, z, "x", (z, 0, 1, h))
        post(FIRST, "free", z)

    def work(at, z):
        while inbox[z]:
            (zs, t, s, h), link = inbox[z].pop(0)
            i = rank[z][zs]
            steps[z].append((tick[z], ("piece", i, t, s, h)))
            piece = (zs, t, s, h)
            if link in ("up", "down"):
                along(at, z, zs, piece) if zs != z else None
                send(at, z, "y", piece)
                send(at, z, "x", piece)
            elif link == "y" and t == 0 and y_first(i, Z):
                send(at, z, "x", piece)
            elif link == "x" and s == 0 and i and not y_first(i, Z):
                send(at, z, "y", piece)
            left[z][i, t] -= 1
            post(at + CORE_LATE, "core", z, (i, t))
        n = tick[z]
        if n < TI:
            tick[z] += 1
            post(max(at + TICK, OWN_END * (n + 1) / TI), "free", z)
            return
        if n % TI == 0:
            ready = [g for g in left[z] if left[z][g] == 0 and g not in order[z]]
            if not ready:
                idle[z] = True
                return
            order[z].append(ready[0])
            steps[z].append((n, ("core",) + ready[0]))
        tick[z] += 1
        post(at + TICK, "free", z)

    while heap:
        at, _, what = heapq.heappop(heap)
        z = what[1]
        if what[0] == "piece":
            inbox[z].append(what[2:])
        elif what[0] == "core":
            left[z][what[2]] -= 1
        if what[0] == "free" or idle[z]:
            if len(order[z]) == 2 * Z and tick[z] == 2 * Z * TI:
                continue
            idle[z] = False
            work(at, z)
    return [(order[z], steps[z]) for z in roles]


def kernel(Z, X, Y, H, tok, cols, TN, U,
           hid_ref, w_ref, tgt_ref, len_ref, lab_ref, dw_ref,
           out_ref,
           buf, w_buf, lg, off_ref, m_ref, s_ref, p_ref,
           stat_out, stat_in, dom_out, dom_in,
           own_sem, in_sem, w_sem, recv_sem, send_sem, st_send, st_recv, dm_send, dm_recv):
    nv = Y * CORES
    dp = Z * X
    ndev = dp * nv
    T = cols // TN
    TI = T // U
    NG = Z * X
    pr = tok // (nv * H)
    me = lax.axis_index("dp")
    v = lax.axis_index("vocab")
    z, x = me // X, me % X
    y, c = v // CORES, v % CORES

    own_copy = pltpu.make_async_copy(hid_ref, buf.at[pl.ds(pl.multiple_of(me * tok, tok), tok)], own_sem)
    own_copy.start()

    def w_copy(j):
        return pltpu.make_async_copy(
            w_ref.at[:, pl.ds(pl.multiple_of(j * TN, TN), TN)], w_buf.at[j], w_sem.at[j]
        )

    for j in range(T):
        w_copy(j).start(priority=1)

    bar = pltpu.get_barrier_semaphore()

    def signal(cond, sem, *at):
        def go():
            pl.semaphore_signal(sem, inc=1, device_id=(at[0] * X + at[1], at[2] * CORES + at[3]),
                                device_id_type=pl.DeviceIdType.MESH)
        if cond is None:
            go()
        else:
            pl.when(cond)(go)
        return 1 if cond is None else jnp.where(cond, 1, 0)

    lines = ((Y, y, lambda q: (z, x, q, c)), (X, x, lambda q: (z, q, y, c)), (Z, z, lambda q: (q, x, y, c)))

    def both(sem, n, pos, at):
        return signal(pos + 1 < n, sem, *at(pos + 1)) + signal(pos > 0, sem, *at(pos - 1))

    near = signal(None, bar, z, x, y, 1 - c)
    for n, pos, at in lines:
        near = near + both(bar, n, pos, at)

    rounds = [None] + [line for line in lines for _ in range(line[0] - 1)]

    def tell(r):
        if rounds[r] is None:
            return signal(None, in_sem.at[r], z, x, y, 1 - c)
        return both(in_sem.at[r], *rounds[r])

    def know(r):
        n = 1
        if rounds[r] is not None:
            size, pos, _ = rounds[r]
            n = jnp.where(pos + 1 < size, 1, 0) + jnp.where(pos > 0, 1, 0)
        pl.semaphore_wait(in_sem.at[r], n)
        if r + 1 < len(rounds):
            tell(r + 1)

    def remote(kind, zs, xs, ys, cs, h, to):
        piece = (((zs * X + xs) * Y + ys) * CORES + cs) * H + h
        rows = buf.at[pl.ds(pl.multiple_of(piece * pr, pr), pr)]
        return pltpu.make_async_remote_copy(
            src_ref=rows, dst_ref=rows,
            send_sem=send_sem.at[kind, piece], recv_sem=recv_sem.at[piece],
            device_id=to, device_id_type=pl.DeviceIdType.MESH,
        )

    def push(drain, cond, *what):
        def go():
            r = remote(*what)
            if drain:
                r.wait_send()
            else:
                r.start()
        if cond is None:
            go()
        else:
            pl.when(cond)(go)

    def dev(z_, x_, y_, c_):
        return (z_ * X + x_, y_ * CORES + c_)

    def arrive(drain, zs, xs, ys, cs, h):
        if not drain:
            remote(0, zs, xs, ys, cs, h, dev(z, x, y, 1 - c)).wait_recv()

    def line(drain, kind, n, pos, src, at, piece):
        if n == 1:
            return
        up, down = pos + 1 < n, pos > 0
        if src is not None:
            if n == 2:
                return
            up, down = up & (src < pos), down & (src > pos)
        if n == 2:
            push(drain, None, kind, *piece, at(1 - pos))
            return
        push(drain, up, kind, *piece, at(pos + 1))
        push(drain, down, kind + 1, *piece, at(pos - 1))

    def send_z(drain, src, piece):
        line(drain, 1, Z, z, src, lambda q: dev(q, x, y, c), piece)

    def send_x(drain, src, piece):
        line(drain, 3, X, x, src, lambda q: dev(z, q, y, c), piece)

    def send_y(drain, src, piece):
        line(drain, 5, Y, y, src, lambda q: dev(z, x, q, c), piece)

    def send_c(drain, piece):
        push(drain, None, 0, *piece, dev(z, x, y, 1 - c))

    def begin(drain):
        for h in range(H):
            send_z(drain, None, (z, x, y, c, h))
            send_x(drain, None, (z, x, y, c, h))
        for k in range(1, Y):
            for h in range(H):
                send_x(drain, None, (z, x, nearest(y, k, Y), c, h))

    def piece_step(drain, i, t, s, h):
        zs, xs, ys = nearest(z, i, Z), nearest(x, t, X), nearest(y, s, Y)
        piece = (zs, xs, ys, c, h)
        arrive(drain, *piece)
        if t == 0 and s == 0:
            send_z(drain, zs, piece)
            send_y(drain, None, piece)
            send_x(drain, None, piece)
        elif t == 0:
            send_y(drain, ys, piece)
            if y_first(i, Z):
                send_x(drain, None, piece)
        elif s == 0:
            send_x(drain, xs, piece)
            if not y_first(i, Z):
                send_y(drain, None, piece)
        elif y_first(i, Z):
            send_x(drain, xs, piece)
        else:
            send_y(drain, ys, piece)
        send_c(drain, piece)

    def core_step(drain, i, t):
        zs, xs = nearest(z, i, Z), nearest(x, t, X)
        for ys in range(Y):
            for h in range(H):
                arrive(drain, zs, xs, ys, 1 - c, h)

    def run(drain, what):
        kind, *at = what
        (piece_step if kind == "piece" else core_step)(drain, *at)

    plans = plan(Z, X, Y, H, TI)
    role = jnp.minimum(z, Z - 1 - z)
    ids = [nearest(z, i, Z) * X + nearest(x, t, X) for i, t in plans[0][0]]
    for r in range(1, len(plans)):
        ids = [jnp.where(role == r, nearest(z, i, Z) * X + nearest(x, t, X), g)
               for (i, t), g in zip(plans[r][0], ids)]

    def take(q):
        def at_tick(whats):
            for what in whats:
                run(False, what)

        def of_role(steps):
            for at in sorted({at for at, _ in steps}):
                pl.when(q == at)(functools.partial(at_tick, [w for n, w in steps if n == at]))

        if all(p == plans[0] for p in plans):
            of_role(plans[0][1])
        else:
            for r, (_, steps) in enumerate(plans):
                pl.when(role == r)(functools.partial(of_role, steps))

    def group(k):
        g = ids[0]
        for n in range(1, NG):
            g = jnp.where(k == n, ids[n], g)
        return g

    col_start = (me * nv + v) * cols
    lane_t = lax.broadcasted_iota(jnp.int32, (LANES, LANES), 1)
    for g in range(dp * tok // LANES):
        rows = pl.ds(g * LANES, LANES)
        ids_row = jnp.broadcast_to(tgt_ref[g:g + 1, :], (LANES, LANES))
        off_ref[rows, :] = jnp.transpose(ids_row) - lane_t - col_start
    m_ref[...] = jnp.full(m_ref.shape, LOW, jnp.float32)
    s_ref[...] = jnp.zeros(s_ref.shape, jnp.float32)
    p_ref[...] = jnp.zeros(p_ref.shape, jnp.float32)
    lg[U - 1] = jnp.full((tok, TN), 3 * LOW, jnp.float32)

    pl.semaphore_wait(bar, near)
    own_copy.wait()
    begin(False)
    tell(0)
    spread = 2 * TI >= len(rounds)

    if not spread:
        for r in range(len(rounds)):
            know(r)

    def epilogue(slot, g, col):
        rows = pl.ds(pl.multiple_of(g * tok, tok), tok)
        off = off_ref[rows, :] - col
        m_old = m_ref[rows, :]
        parts = [lg[slot, :, n * LANES:(n + 1) * LANES] for n in range(TN // LANES)]
        m_new = m_old
        for a in parts:
            m_new = jnp.maximum(m_new, a)
        s = s_ref[rows, :] * jnp.exp(m_old - m_new)
        pk = p_ref[rows, :]
        for n, a in enumerate(parts):
            s = s + jnp.exp(a - m_new)
            pk = pk + jnp.where(off == n * LANES, a, 0.0)
        m_ref[rows, :] = m_new
        s_ref[rows, :] = s
        p_ref[rows, :] = pk

    row8 = lax.broadcasted_iota(jnp.int32, (8, tok), 0)

    def finish(g):
        rows = pl.ds(pl.multiple_of(g * tok, tok), tok)
        mt = jnp.transpose(m_ref[rows, :])
        st = jnp.transpose(s_ref[rows, :])
        pt = jnp.transpose(p_ref[rows, :])
        row_m = jnp.max(mt, axis=0, keepdims=True)
        row_s = jnp.sum(st * jnp.exp(mt - row_m), axis=0, keepdims=True)
        row_p = jnp.sum(pt, axis=0, keepdims=True)
        stat_out[g] = jnp.where(row8 == 0, row_m, jnp.where(row8 == 1, row_s, row_p))

        @pl.when(g == me)
        def _():
            stat_in[me * nv + v] = stat_out[me]

        for k in range(nv):
            @pl.when((g != me) | (v != k))
            def _():
                pltpu.make_async_remote_copy(
                    src_ref=stat_out.at[g], dst_ref=stat_in.at[me * nv + v],
                    send_sem=st_send, recv_sem=st_recv,
                    device_id=(g, k), device_id_type=pl.DeviceIdType.MESH,
                ).start()

    def tick(q, _):
        k = q // TI
        i = q - k * TI
        if spread:
            for r in range(len(rounds)):
                pl.when(q == r + 1)(functools.partial(know, r))
        take(q)

        @pl.when(k == 0)
        def _():
            for u in range(U):
                w_copy(i * U + u).wait()

        @pl.when(((q - 1) % TI == 0) & (q > TI))
        def _():
            finish(group((q - 1) // TI - 1))

        g = group(k)
        rows = pl.ds(pl.multiple_of(g * tok, tok), tok)
        for u in range(U):
            j = i * U + u
            if u == 0:
                g_old = jnp.where(i == 0, group(jnp.maximum(k - 1, 0)), g)
                col = jnp.where(q == 0, -(1 << 30), jnp.where(i == 0, (T - 1) * TN, (j - 1) * TN))
                epilogue(U - 1, g_old, col)
            else:
                epilogue(u - 1, g, (j - 1) * TN)
            lg[u] = jnp.dot(buf[rows, :], w_buf[j], preferred_element_type=jnp.float32)
        return 0

    lax.fori_loop(0, NG * TI, tick, 0)
    epilogue(U - 1, ids[NG - 1], (T - 1) * TN)
    for k in range(NG):
        if (k + 1) * TI + 1 >= NG * TI:
            finish(ids[k])

    begin(True)
    for _, what in plans[0][1]:
        run(True, what)

    seq = lax.broadcasted_iota(jnp.int32, (1, tok), 1)
    lens = jnp.zeros((1, tok), jnp.int32)
    labs = jnp.zeros((1, tok), jnp.int32)
    for n in range(tok // SEQ_LEN):
        mine = seq // SEQ_LEN == n
        lens = jnp.where(mine, len_ref[n], lens)
        labs = jnp.where(mine, lab_ref[n], labs)
    valid = seq % SEQ_LEN < lens
    hot = lax.broadcasted_iota(jnp.int32, (LANES, tok), 0) == labs
    d_count = jnp.sum(jnp.where(hot & valid, 1.0, 0.0), axis=1, keepdims=True)
    dlane = lax.broadcasted_iota(jnp.int32, (LANES, LANES), 1)
    counts = jnp.where(dlane == 1, d_count, 0.0)
    dom = lax.broadcasted_iota(jnp.int32, (1, LANES), 1)
    live = dom < DOMAINS
    weights = jnp.zeros((1, LANES), jnp.float32)
    for n in range(DOMAINS):
        weights = jnp.where(dom == n, dw_ref[n], weights)
    probability = (1.0 - DOMAINS * explore_share) * weights / jnp.sum(
        weights, axis=1, keepdims=True) + explore_share

    others = stat_in.at[pl.ds(0, ndev - 1)]
    pltpu.make_async_copy(others, others, st_recv).wait()
    ms = stat_in[:, 0, :]
    peak = jnp.max(ms, axis=0, keepdims=True)
    mass = jnp.sum(stat_in[:, 1, :] * jnp.exp(ms - peak), axis=0, keepdims=True)
    pick = jnp.sum(stat_in[:, 2, :], axis=0, keepdims=True)
    loss = jnp.where(valid, jnp.log(mass) + peak - pick, 0.0)
    d_loss = jnp.sum(jnp.where(hot, loss, 0.0), axis=1, keepdims=True)
    dom_out[...] = jnp.transpose(jnp.where(dlane == 0, d_loss, counts))[:8]
    for k in range(1, dp):
        pltpu.make_async_remote_copy(
            src_ref=dom_out, dst_ref=dom_in.at[me],
            send_sem=dm_send, recv_sem=dm_recv,
            device_id=((me + k) % dp, v), device_id_type=pl.DeviceIdType.MESH,
        ).start()
    dom_in[me] = dom_out[...]
    out_ref[0:1, :] = loss
    pltpu.make_async_copy(others, others, st_send).wait()

    rest = dom_in.at[pl.ds(0, dp - 1)]
    pltpu.make_async_copy(rest, rest, dm_recv).wait()
    total = jnp.sum(dom_in[...], axis=0)
    reward = total[0:1] / jnp.maximum(total[1:2], 1.0) / probability
    raised = jnp.where(live, weights * jnp.exp(step_rate * reward), 0.0)
    out_ref[1:2, :] = DOMAINS * raised / jnp.sum(raised, axis=1, keepdims=True)
    pltpu.make_async_copy(rest, rest, dm_send).wait()


def body(hidden_states, head_weight, target_ids, seq_lengths, domain_labels, domain_weights):
    tok, width = hidden_states.shape
    cols = head_weight.shape[1]
    dp = lax.axis_size("dp")
    nv = lax.axis_size("vocab")
    X = math.isqrt(dp // 2)
    Z = dp // X
    Y = nv // CORES
    tokens = dp * tok
    TN = next(n for n in (4 * LANES, 3 * LANES, 2 * LANES, LANES) if cols % n == 0)
    T = cols // TN
    U = 2 if T % 2 == 0 else 1
    H = HALVES if tok // (nv * HALVES) >= 16 else 1
    hbm = pl.BlockSpec(memory_space=pl.ANY)
    vmem = pl.BlockSpec(memory_space=pltpu.VMEM)
    smem = pl.BlockSpec(memory_space=pltpu.SMEM)
    f32 = jnp.float32
    dma = pltpu.SemaphoreType.DMA
    out = pl.pallas_call(
        functools.partial(kernel, Z, X, Y, H, tok, cols, TN, U),
        out_shape=jax.ShapeDtypeStruct((2, tok), f32),
        in_specs=[hbm, hbm, vmem, smem, smem, smem],
        out_specs=vmem,
        scratch_shapes=[
            pltpu.VMEM((tokens, width), hidden_states.dtype),
            pltpu.VMEM((T, width, TN), head_weight.dtype),
            pltpu.VMEM((U, tok, TN), f32),
            pltpu.VMEM((tokens, LANES), jnp.int32),
            pltpu.VMEM((tokens, LANES), f32),
            pltpu.VMEM((tokens, LANES), f32),
            pltpu.VMEM((tokens, LANES), f32),
            pltpu.VMEM((dp, 8, tok), f32),
            pltpu.VMEM((dp * nv, 8, tok), f32),
            pltpu.VMEM((8, LANES), f32),
            pltpu.VMEM((dp, 8, LANES), f32),
            dma(()),
            pltpu.SemaphoreType.REGULAR((1 + X + Y + Z - 3,)),
            dma((T,)),
            dma((dp * nv * H,)),
            dma((7, dp * nv * H)),
            dma(()), dma(()), dma(()), dma(()),
        ],
        compiler_params=pltpu.CompilerParams(
            has_side_effects=True, collective_id=0, vmem_limit_bytes=60 * 2**20),
    )(hidden_states, head_weight, target_ids.reshape(tokens // LANES, LANES), seq_lengths, domain_labels,
      domain_weights)
    return out[0], out[1, :DOMAINS]


def solution(mesh):
    placed = (P("dp", None), P(None, ("dp", "vocab")), P(), P("dp"), P("dp"), P())
    return jax.shard_map(
        body, mesh=mesh, in_specs=placed, out_specs=(P("dp"), P()), check_vma=False
    )
```

```python
import functools
import heapq
import math
import random

import jax
import jax.numpy as jnp
from jax import lax
from jax.experimental import pallas as pl
from jax.experimental.pallas import tpu as pltpu
from jax.sharding import PartitionSpec as P

SEQ_LEN = 16
DOMAINS = 22
LANES = 128
CORES = 2
LOW = -1e30
HALVES = 1

explore_share = 0.01
step_rate = 0.002


def nearest(p, i, n):
    if isinstance(p, int):
        q = min(p, n - 1 - p)
        k = (i + 1) // 2
        at = i if i > 2 * q else q + k if i % 2 else q - k
        return at if p == q else n - 1 - at
    if i == 0:
        return p
    if n == 2:
        return 1 - p
    q = jnp.minimum(p, n - 1 - p)
    k = (i + 1) // 2
    at = jnp.where(i > 2 * q, i, q + k if i % 2 else q - k)
    return jnp.where(p == q, at, n - 1 - at)


WIRE, LATE, CORE_LATE, TICK, FIRST, OWN_END, START = 4.92, 2.2, 1.6, 1.14, 3.0, 9.0, 3.5
TRIES = 3000


def far_first(Z, X, Y, H, TI):
    order = sorted(((i, t) for i in range(Z) for t in range(X)), key=lambda g: (2 * g[0] + 3 * g[1], g))
    steps = []
    for k, (i, t) in enumerate(order):
        if k:
            steps += [(k * TI, ("piece", i, t, s, h)) for s in range(Y) for h in range(H)]
            steps.append((k * TI, ("core", i, t)))
    return order, steps


def targets(Z, route, z, zs, t, s):
    def inbound(w, t, s):
        i = next(i for i in range(Z) if nearest(w, i, Z) == zs)
        return route[min(w, Z - 1 - w)].get((i, t, s))

    out = []
    for w, link in ((z + 1, "up"), (z - 1, "down")):
        if 0 <= w < Z and abs(w - zs) > abs(z - zs) and inbound(w, t, s) == "z":
            out.append((link, w, (zs, t, s)))
    if inbound(z, t, 1 - s) == "y":
        out.append(("y", z, (zs, t, 1 - s)))
    if inbound(z, 1 - t, s) == "x":
        out.append(("x", z, (zs, 1 - t, s)))
    return out


def first_sends(Z, route, z):
    return [(s, [e for e in targets(Z, route, z, z, 0, s) if e[0] != "y"]) for s in (0, 1)]


def model(Z, H, TI, route):
    rank = [{nearest(z, i, Z): i for i in range(Z)} for z in range(Z)]
    onward = {(z, zs, t, s): targets(Z, route, z, zs, t, s)
              for z in range(Z) for zs in range(Z) for t in (0, 1) for s in (0, 1)}
    heap, free, got = [], {}, set()
    count = [0]

    def post(at, *what):
        count[0] += 1
        heapq.heappush(heap, (at, count[0], what))

    def send(at, z, link, to, piece):
        free[z, link] = max(at, free.get((z, link), 0.0)) + WIRE / H
        post(free[z, link] + LATE, "piece", to, piece)

    inbox = [[] for _ in range(Z)]
    left = [{(i, t): 4 * H for i in range(Z) for t in range(2) if i or t} for _ in range(Z)]
    order = [[(0, 0)] for _ in range(Z)]
    steps = [[] for _ in range(Z)]
    tick, idle, end = [0] * Z, [False] * Z, [0.0] * Z
    total = 2 * Z * TI
    for z in range(Z):
        for s, sends in first_sends(Z, route, z):
            for h in range(H):
                for link, w, to in sends:
                    send(START, z, link, w, to + (h,))
        post(FIRST, "free", z)

    def work(at, z):
        while inbox[z]:
            piece = inbox[z].pop(0)
            if (z, piece) in got:
                return
            got.add((z, piece))
            zs, t, s, h = piece
            i = rank[z][zs]
            steps[z].append((tick[z], ("piece", i, t, s, h)))
            for link, w, to in onward[z, zs, t, s]:
                send(at, z, link, w, to + (h,))
            left[z][i, t] -= 1
            post(at + CORE_LATE, "core", z, (i, t))
        n = tick[z]
        if n < TI:
            tick[z] += 1
            post(max(at + TICK, OWN_END * (n + 1) / TI), "free", z)
            return
        if n % TI == 0:
            ready = [g for g in left[z] if left[z][g] == 0 and g not in order[z]]
            if not ready:
                idle[z] = True
                return
            order[z].append(ready[0])
            steps[z].append((n, ("core",) + ready[0]))
        tick[z] += 1
        end[z] = at + TICK
        post(at + TICK, "free", z)

    while heap:
        at, _, what = heapq.heappop(heap)
        z = what[1]
        if what[0] == "piece":
            inbox[z].append(what[2])
        elif what[0] == "core":
            left[z][what[2]] -= 1
        if (what[0] == "free" or idle[z]) and tick[z] < total:
            idle[z] = False
            work(at, z)
    full = all(n == total for n in tick)
    return (round(max(end), 2) if full else 1e9, sum(end)), order, steps


@functools.cache
def plan(Z, H, TI):
    roles = range((Z + 1) // 2)
    best = []
    for _ in roles:
        links = {(0, 1, 0): "x", (0, 1, 1): "x"}
        for i in range(1, Z):
            last = "x" if i in (1, Z - 1) else "y"
            links.update({(i, 0, 0): "z", (i, 0, 1): "y", (i, 1, 0): "x", (i, 1, 1): last})
        best.append(links)
    draw = random.Random(SEED)
    at = best
    score = at_score = model(Z, H, TI, best)[0]
    for _ in range(TRIES):
        trial = [dict(links) for links in at]
        for _ in range(draw.choice((1, 1, 2, 3))):
            links = draw.choice(trial)
            key = draw.choice(sorted(links))
            links[key] = draw.choice("xy" if key[0] == 0 else "zy" if key[1] == 0 else "zxy")
        got = model(Z, H, TI, trial)[0]
        if got <= at_score or draw.random() < math.exp(max(-60.0, (at_score[0] - got[0]) / 0.3)):
            at, at_score = trial, got
        if got < score:
            best, score = trial, got
    _, order, steps = model(Z, H, TI, best)
    return best, order, steps


SEED = 1


def kernel(Z, X, Y, H, tok, cols, TN, U,
           hid_ref, w_ref, tgt_ref, len_ref, lab_ref, dw_ref,
           out_ref,
           buf, w_buf, lg, off_ref, m_ref, s_ref, p_ref,
           stat_out, stat_in, dom_out, dom_in,
           own_sem, in_sem, w_sem, recv_sem, send_sem, st_send, st_recv, dm_send, dm_recv):
    nv = Y * CORES
    dp = Z * X
    ndev = dp * nv
    T = cols // TN
    TI = T // U
    NG = Z * X
    pr = tok // (nv * H)
    me = lax.axis_index("dp")
    v = lax.axis_index("vocab")
    z, x = me // X, me % X
    y, c = v // CORES, v % CORES

    own_copy = pltpu.make_async_copy(hid_ref, buf.at[pl.ds(pl.multiple_of(me * tok, tok), tok)], own_sem)
    own_copy.start()

    def w_copy(j):
        return pltpu.make_async_copy(
            w_ref.at[:, pl.ds(pl.multiple_of(j * TN, TN), TN)], w_buf.at[j], w_sem.at[j]
        )

    for j in range(T):
        w_copy(j).start(priority=1)

    bar = pltpu.get_barrier_semaphore()

    def signal(cond, sem, *at):
        def go():
            pl.semaphore_signal(sem, inc=1, device_id=(at[0] * X + at[1], at[2] * CORES + at[3]),
                                device_id_type=pl.DeviceIdType.MESH)
        if cond is None:
            go()
        else:
            pl.when(cond)(go)
        return 1 if cond is None else jnp.where(cond, 1, 0)

    lines = ((Y, y, lambda q: (z, x, q, c)), (X, x, lambda q: (z, q, y, c)), (Z, z, lambda q: (q, x, y, c)))

    def both(sem, n, pos, at):
        return signal(pos + 1 < n, sem, *at(pos + 1)) + signal(pos > 0, sem, *at(pos - 1))

    near = signal(None, bar, z, x, y, 1 - c)
    for n, pos, at in lines:
        near = near + both(bar, n, pos, at)

    rounds = [None] + [line for line in lines for _ in range(line[0] - 1)]

    def tell(r):
        if rounds[r] is None:
            return signal(None, in_sem.at[r], z, x, y, 1 - c)
        return both(in_sem.at[r], *rounds[r])

    def know(r):
        n = 1
        if rounds[r] is not None:
            size, pos, _ = rounds[r]
            n = jnp.where(pos + 1 < size, 1, 0) + jnp.where(pos > 0, 1, 0)
        pl.semaphore_wait(in_sem.at[r], n)
        if r + 1 < len(rounds):
            tell(r + 1)

    def remote(kind, zs, xs, ys, cs, h, to):
        piece = (((zs * X + xs) * Y + ys) * CORES + cs) * H + h
        rows = buf.at[pl.ds(pl.multiple_of(piece * pr, pr), pr)]
        return pltpu.make_async_remote_copy(
            src_ref=rows, dst_ref=rows,
            send_sem=send_sem.at[kind, piece], recv_sem=recv_sem.at[piece],
            device_id=to, device_id_type=pl.DeviceIdType.MESH,
        )

    def push(drain, cond, *what):
        def go():
            r = remote(*what)
            if drain:
                r.wait_send()
            else:
                r.start()
        if cond is None:
            go()
        else:
            pl.when(cond)(go)

    def dev(z_, x_, y_, c_):
        return (z_ * X + x_, y_ * CORES + c_)

    def arrive(drain, zs, xs, ys, cs, h):
        if not drain:
            remote(0, zs, xs, ys, cs, h, dev(z, x, y, 1 - c)).wait_recv()

    def line(drain, kind, n, pos, src, at, piece):
        if n == 1:
            return
        up, down = pos + 1 < n, pos > 0
        if src is not None:
            if n == 2:
                return
            up, down = up & (src < pos), down & (src > pos)
        if n == 2:
            push(drain, None, kind, *piece, at(1 - pos))
            return
        push(drain, up, kind, *piece, at(pos + 1))
        push(drain, down, kind + 1, *piece, at(pos - 1))

    def send_z(drain, src, piece):
        line(drain, 1, Z, z, src, lambda q: dev(q, x, y, c), piece)

    def send_x(drain, src, piece):
        line(drain, 3, X, x, src, lambda q: dev(z, q, y, c), piece)

    def send_y(drain, src, piece):
        line(drain, 5, Y, y, src, lambda q: dev(z, x, q, c), piece)

    def send_c(drain, piece):
        push(drain, None, 0, *piece, dev(z, x, y, 1 - c))

    flat = X == 2 and Y == 2
    roles = range((Z + 1) // 2) if flat else range(1)
    role = jnp.minimum(z, Z - 1 - z)
    if flat:
        route, orders, all_steps = plan(Z, H, TI)
    else:
        order, steps = far_first(Z, X, Y, H, TI)
        orders, all_steps = [order], [steps]

    def by_links(drain, sends, piece):
        low = z + z <= Z - 1
        inward = jnp.where(low, 1, -1)
        for link, _, _ in sends:
            if link == "x":
                push(drain, None, 3, *piece, dev(z, 1 - x, y, c))
            elif link == "y":
                push(drain, None, 5, *piece, dev(z, x, 1 - y, c))
            elif link == "up":
                push(drain, None, 1, *piece, dev(z + inward, x, y, c))
            else:
                push(drain, None, 2, *piece, dev(z - inward, x, y, c))

    def begin(drain, r):
        if flat:
            for s, sends in first_sends(Z, route, r):
                for h in range(H):
                    by_links(drain, sends, (z, x, nearest(y, s, Y), c, h))
            return
        for h in range(H):
            send_z(drain, None, (z, x, y, c, h))
            send_x(drain, None, (z, x, y, c, h))
        for k in range(1, Y):
            for h in range(H):
                send_x(drain, None, (z, x, nearest(y, k, Y), c, h))

    def piece_step(drain, r, i, t, s, h):
        zs, xs, ys = nearest(z, i, Z), nearest(x, t, X), nearest(y, s, Y)
        piece = (zs, xs, ys, c, h)
        arrive(drain, *piece)
        if flat:
            by_links(drain, targets(Z, route, r, nearest(r, i, Z), t, s), piece)
        elif t == 0 and s == 0:
            send_z(drain, zs, piece)
            send_y(drain, None, piece)
            send_x(drain, None, piece)
        elif t == 0:
            send_y(drain, ys, piece)
            send_x(drain, None, piece)
        else:
            send_x(drain, xs, piece)
        send_c(drain, piece)

    def core_step(drain, r, i, t):
        zs, xs = nearest(z, i, Z), nearest(x, t, X)
        for ys in range(Y):
            for h in range(H):
                arrive(drain, zs, xs, ys, 1 - c, h)

    def run(drain, r, what):
        kind, *at = what
        (piece_step if kind == "piece" else core_step)(drain, r, *at)

    def by_role(what):
        for r in roles:
            if len(roles) == 1:
                what(r)
            else:
                pl.when(role == r)(functools.partial(what, r))

    ids = [nearest(z, i, Z) * X + nearest(x, t, X) for i, t in orders[0]]
    for r in roles[1:]:
        ids = [jnp.where(role == r, nearest(z, i, Z) * X + nearest(x, t, X), g) for (i, t), g in zip(orders[r], ids)]

    def take(q):
        def at_tick(r, whats):
            for what in whats:
                run(False, r, what)

        def of_role(r):
            for at in sorted({at for at, _ in all_steps[r]}):
                pl.when(q == at)(functools.partial(at_tick, r, [w for n, w in all_steps[r] if n == at]))

        by_role(of_role)

    def drain_role(r):
        begin(True, r)
        for _, what in all_steps[r]:
            run(True, r, what)

    def group(k):
        g = ids[0]
        for n in range(1, NG):
            g = jnp.where(k == n, ids[n], g)
        return g

    col_start = (me * nv + v) * cols
    lane_t = lax.broadcasted_iota(jnp.int32, (LANES, LANES), 1)
    for g in range(dp * tok // LANES):
        rows = pl.ds(g * LANES, LANES)
        ids_row = jnp.broadcast_to(tgt_ref[g:g + 1, :], (LANES, LANES))
        off_ref[rows, :] = jnp.transpose(ids_row) - lane_t - col_start
    m_ref[...] = jnp.full(m_ref.shape, LOW, jnp.float32)
    s_ref[...] = jnp.zeros(s_ref.shape, jnp.float32)
    p_ref[...] = jnp.zeros(p_ref.shape, jnp.float32)
    lg[U - 1] = jnp.full((tok, TN), 3 * LOW, jnp.float32)

    pl.semaphore_wait(bar, near)
    own_copy.wait()
    by_role(functools.partial(begin, False))
    tell(0)
    spread = 2 * TI >= len(rounds)

    if not spread:
        for r in range(len(rounds)):
            know(r)

    def epilogue(slot, g, col):
        rows = pl.ds(pl.multiple_of(g * tok, tok), tok)
        off = off_ref[rows, :] - col
        m_old = m_ref[rows, :]
        parts = [lg[slot, :, n * LANES:(n + 1) * LANES] for n in range(TN // LANES)]
        m_new = m_old
        for a in parts:
            m_new = jnp.maximum(m_new, a)
        s = s_ref[rows, :] * jnp.exp(m_old - m_new)
        pk = p_ref[rows, :]
        for n, a in enumerate(parts):
            s = s + jnp.exp(a - m_new)
            pk = pk + jnp.where(off == n * LANES, a, 0.0)
        m_ref[rows, :] = m_new
        s_ref[rows, :] = s
        p_ref[rows, :] = pk

    row8 = lax.broadcasted_iota(jnp.int32, (8, tok), 0)

    def finish(g):
        rows = pl.ds(pl.multiple_of(g * tok, tok), tok)
        mt = jnp.transpose(m_ref[rows, :])
        st = jnp.transpose(s_ref[rows, :])
        pt = jnp.transpose(p_ref[rows, :])
        row_m = jnp.max(mt, axis=0, keepdims=True)
        row_s = jnp.sum(st * jnp.exp(mt - row_m), axis=0, keepdims=True)
        row_p = jnp.sum(pt, axis=0, keepdims=True)
        stat_out[g] = jnp.where(row8 == 0, row_m, jnp.where(row8 == 1, row_s, row_p))

        @pl.when(g == me)
        def _():
            stat_in[me * nv + v] = stat_out[me]

        for k in range(nv):
            @pl.when((g != me) | (v != k))
            def _():
                pltpu.make_async_remote_copy(
                    src_ref=stat_out.at[g], dst_ref=stat_in.at[me * nv + v],
                    send_sem=st_send, recv_sem=st_recv,
                    device_id=(g, k), device_id_type=pl.DeviceIdType.MESH,
                ).start()

    def tick(q, _):
        k = q // TI
        i = q - k * TI
        if spread:
            for r in range(len(rounds)):
                pl.when(q == r + 1)(functools.partial(know, r))
        take(q)

        @pl.when(k == 0)
        def _():
            for u in range(U):
                w_copy(i * U + u).wait()

        @pl.when(((q - 1) % TI == 0) & (q > TI))
        def _():
            finish(group((q - 1) // TI - 1))

        g = group(k)
        rows = pl.ds(pl.multiple_of(g * tok, tok), tok)
        for u in range(U):
            j = i * U + u
            if u == 0:
                g_old = jnp.where(i == 0, group(jnp.maximum(k - 1, 0)), g)
                col = jnp.where(q == 0, -(1 << 30), jnp.where(i == 0, (T - 1) * TN, (j - 1) * TN))
                epilogue(U - 1, g_old, col)
            else:
                epilogue(u - 1, g, (j - 1) * TN)
            lg[u] = jnp.dot(buf[rows, :], w_buf[j], preferred_element_type=jnp.float32)
        return 0

    lax.fori_loop(0, NG * TI, tick, 0)
    epilogue(U - 1, ids[NG - 1], (T - 1) * TN)
    for k in range(NG):
        if (k + 1) * TI + 1 >= NG * TI:
            finish(ids[k])

    by_role(drain_role)

    seq = lax.broadcasted_iota(jnp.int32, (1, tok), 1)
    lens = jnp.zeros((1, tok), jnp.int32)
    labs = jnp.zeros((1, tok), jnp.int32)
    for n in range(tok // SEQ_LEN):
        mine = seq // SEQ_LEN == n
        lens = jnp.where(mine, len_ref[n], lens)
        labs = jnp.where(mine, lab_ref[n], labs)
    valid = seq % SEQ_LEN < lens
    hot = lax.broadcasted_iota(jnp.int32, (LANES, tok), 0) == labs
    d_count = jnp.sum(jnp.where(hot & valid, 1.0, 0.0), axis=1, keepdims=True)
    dlane = lax.broadcasted_iota(jnp.int32, (LANES, LANES), 1)
    counts = jnp.where(dlane == 1, d_count, 0.0)
    dom = lax.broadcasted_iota(jnp.int32, (1, LANES), 1)
    live = dom < DOMAINS
    weights = jnp.zeros((1, LANES), jnp.float32)
    for n in range(DOMAINS):
        weights = jnp.where(dom == n, dw_ref[n], weights)
    probability = (1.0 - DOMAINS * explore_share) * weights / jnp.sum(
        weights, axis=1, keepdims=True) + explore_share

    others = stat_in.at[pl.ds(0, ndev - 1)]
    pltpu.make_async_copy(others, others, st_recv).wait()
    ms = stat_in[:, 0, :]
    peak = jnp.max(ms, axis=0, keepdims=True)
    mass = jnp.sum(stat_in[:, 1, :] * jnp.exp(ms - peak), axis=0, keepdims=True)
    pick = jnp.sum(stat_in[:, 2, :], axis=0, keepdims=True)
    loss = jnp.where(valid, jnp.log(mass) + peak - pick, 0.0)
    d_loss = jnp.sum(jnp.where(hot, loss, 0.0), axis=1, keepdims=True)
    dom_out[...] = jnp.transpose(jnp.where(dlane == 0, d_loss, counts))[:8]
    for k in range(1, dp):
        pltpu.make_async_remote_copy(
            src_ref=dom_out, dst_ref=dom_in.at[me],
            send_sem=dm_send, recv_sem=dm_recv,
            device_id=((me + k) % dp, v), device_id_type=pl.DeviceIdType.MESH,
        ).start()
    dom_in[me] = dom_out[...]
    out_ref[0:1, :] = loss
    pltpu.make_async_copy(others, others, st_send).wait()

    rest = dom_in.at[pl.ds(0, dp - 1)]
    pltpu.make_async_copy(rest, rest, dm_recv).wait()
    total = jnp.sum(dom_in[...], axis=0)
    reward = total[0:1] / jnp.maximum(total[1:2], 1.0) / probability
    raised = jnp.where(live, weights * jnp.exp(step_rate * reward), 0.0)
    out_ref[1:2, :] = DOMAINS * raised / jnp.sum(raised, axis=1, keepdims=True)
    pltpu.make_async_copy(rest, rest, dm_send).wait()


def body(hidden_states, head_weight, target_ids, seq_lengths, domain_labels, domain_weights):
    tok, width = hidden_states.shape
    cols = head_weight.shape[1]
    dp = lax.axis_size("dp")
    nv = lax.axis_size("vocab")
    X = math.isqrt(dp // 2)
    Z = dp // X
    Y = nv // CORES
    tokens = dp * tok
    TN = next(n for n in (4 * LANES, 3 * LANES, 2 * LANES, LANES) if cols % n == 0)
    T = cols // TN
    U = 2 if T % 2 == 0 else 1
    H = HALVES if tok // (nv * HALVES) >= 16 else 1
    hbm = pl.BlockSpec(memory_space=pl.ANY)
    vmem = pl.BlockSpec(memory_space=pltpu.VMEM)
    smem = pl.BlockSpec(memory_space=pltpu.SMEM)
    f32 = jnp.float32
    dma = pltpu.SemaphoreType.DMA
    out = pl.pallas_call(
        functools.partial(kernel, Z, X, Y, H, tok, cols, TN, U),
        out_shape=jax.ShapeDtypeStruct((2, tok), f32),
        in_specs=[hbm, hbm, vmem, smem, smem, smem],
        out_specs=vmem,
        scratch_shapes=[
            pltpu.VMEM((tokens, width), hidden_states.dtype),
            pltpu.VMEM((T, width, TN), head_weight.dtype),
            pltpu.VMEM((U, tok, TN), f32),
            pltpu.VMEM((tokens, LANES), jnp.int32),
            pltpu.VMEM((tokens, LANES), f32),
            pltpu.VMEM((tokens, LANES), f32),
            pltpu.VMEM((tokens, LANES), f32),
            pltpu.VMEM((dp, 8, tok), f32),
            pltpu.VMEM((dp * nv, 8, tok), f32),
            pltpu.VMEM((8, LANES), f32),
            pltpu.VMEM((dp, 8, LANES), f32),
            dma(()),
            pltpu.SemaphoreType.REGULAR((1 + X + Y + Z - 3,)),
            dma((T,)),
            dma((dp * nv * H,)),
            dma((7, dp * nv * H)),
            dma(()), dma(()), dma(()), dma(()),
        ],
        compiler_params=pltpu.CompilerParams(
            has_side_effects=True, collective_id=0, vmem_limit_bytes=60 * 2**20),
    )(hidden_states, head_weight, target_ids.reshape(tokens // LANES, LANES), seq_lengths, domain_labels,
      domain_weights)
    return out[0], out[1, :DOMAINS]


def solution(mesh):
    placed = (P("dp", None), P(None, ("dp", "vocab")), P(), P("dp"), P("dp"), P())
    return jax.shard_map(
        body, mesh=mesh, in_specs=placed, out_specs=(P("dp"), P()), check_vma=False
    )
```
